32 devices in a mesh: row: 4 (over z), col: 4 (over x, core), depth: 2 (over y).
Axes of the slice: x: 2, y: 2, z: 4, core: 2. Of those that a mesh axis runs over, the one named last changes fastest.
Arguments:
- heads_concat: bfloat16 [2048, 16384], P('row', ('depth', 'col')), may hold values from -6 to 6
- w_out: bfloat16 [16384, 7168], P(('depth', 'row'), 'col'), may hold values from -0.046875 to 0.046875
Outputs:
- projected: bfloat16 [2048, 7168], P('row', ('col', 'depth'))
The draws below stay inside these ranges and needn't reach their ends.
All inputs are finite; a program needn't handle non-finite values.
Results may differ from the reference program's by a relative error of at most 0.001.
Values may be sent and summed in bfloat16 or wider, within the bound.
A program may use at most 128 MiB of HBM per device.

```python
import jax
import jax.numpy as jnp

D = 7168
K = 16384
TOKENS = 2048


def block_levels(stream_key, dims, cuts, least, top_value):
    factor_of, own = 1.0, jax.random.fold_in(stream_key, 6)
    for dim, parts in cuts:
        draws = jnp.exp(jax.random.uniform(jax.random.fold_in(own, dim), (parts,), jnp.float32, least / len(cuts), top_value / len(cuts)))
        factor_of = factor_of * jnp.repeat(draws, dims[dim] // parts).reshape([-1 if axis == dim else 1 for axis in range(len(dims))])
    return factor_of


def bell_draw(stream_key, extent, scale, limit, pieces=(), held_as=jnp.bfloat16):
    values = scale * jax.random.normal(stream_key, extent, jnp.float32)
    if pieces:
        values = values * block_levels(stream_key, extent, pieces, -0.22, 0.18)
    return jnp.clip(values, -limit, limit).astype(held_as)


def setup_inputs(seed: int = 0) -> dict:
    key_of = jax.random.split(jax.random.key(seed), 3)
    return {
        "heads_concat": bell_draw(key_of[0], (TOKENS, K), 1.0, 6.0, ((0, 4), (1, 8))),
        "w_out": bell_draw(key_of[1], (K, D), K ** -0.5, 0.046875, ((0, 8), (1, 4))),
    }


def reference(heads_concat, w_out):
    product = jnp.dot(heads_concat, w_out, preferred_element_type=jnp.float32)
    return product.astype(jnp.bfloat16)
```

```python
import functools

import jax
import jax.numpy as jnp
from jax import lax
from jax.experimental import pallas as pl
from jax.experimental.pallas import tpu as pltpu
from jax.sharding import PartitionSpec as P

MESH = pl.DeviceIdType.MESH
CORES = 2
LAG = 4
VMEM_BYTES = 66_000_000


def kernel(rows, cols, aligned, a_ref, w_ref, o_ref, w, a, own, out_y, in_y, chain,
           w_sem, s1_send, s1_recv, x_send, x_recv, c_send, c_recv, f_send, f_recv,
           y_send, y_recv, z_send, z_recv):
    r, j, d = lax.axis_index("row"), lax.axis_index("col"), lax.axis_index("depth")
    chips = cols // CORES
    x, core = j // CORES, j % CORES
    share = rows // cols
    tq, kb = a.shape[2], a.shape[3]
    nh = own.shape[3]
    steps = rows * cols
    mate = {"row": r, "col": x * CORES + 1 - core, "depth": d}
    across = {"row": r, "col": j, "depth": 1 - d}
    below = {"row": lax.rem(r + rows - 1, rows), "col": j, "depth": d}
    above = {"row": lax.rem(r + 1, rows), "col": j, "depth": d}
    source_col = r // share

    def x_col(dx):
        return lax.rem(x + dx, chips) * CORES + core

    def x_peer(dx):
        return {"row": r, "col": x_col(dx), "depth": d}

    w_copy = pltpu.make_async_copy(w_ref, w, w_sem)
    w_copy.start()

    barrier = pltpu.get_barrier_semaphore()

    def greet(device):
        pl.semaphore_signal(barrier, inc=1, device_id=device, device_id_type=MESH)

    for t in range(rows):
        pl.when(jnp.logical_or(r != t, source_col != j))(
            lambda t=t: greet({"row": t, "col": source_col, "depth": d})
        )
    for dx in range(1, chips):
        greet(x_peer(dx))
    greet(mate)
    greet(across)
    pl.when(r > 0)(lambda: greet(below))
    pl.when(r < rows - 1)(lambda: greet(above))
    pl.semaphore_wait(
        barrier,
        share * cols + chips
        + jnp.where(source_col != j, 1, 0)
        + jnp.where(r > 0, 1, 0)
        + jnp.where(r < rows - 1, 1, 0),
    )

    def remote(src, dst, send, recv, device):
        return pltpu.make_async_remote_copy(
            src_ref=src, dst_ref=dst, send_sem=send, recv_sem=recv,
            device_id=device, device_id_type=MESH,
        )

    def first(i, q):
        target = {"row": j * share + i, "col": q, "depth": d}
        source = a_ref.at[pl.ds(q * tq, tq), pl.ds(i * kb, kb)]
        return remote(source, a.at[r, q], s1_send.at[i, q], s1_recv.at[r], target)

    def is_me(i, q):
        return jnp.logical_and(r == j * share + i, j == q)

    for i in range(share):
        for q in range(cols):
            @pl.when(is_me(i, q))
            def _():
                pltpu.make_async_copy(
                    a_ref.at[pl.ds(q * tq, tq), pl.ds(i * kb, kb)],
                    a.at[r, q], s1_recv.at[r],
                ).start()

            @pl.when(jnp.logical_not(is_me(i, q)))
            def _():
                first(i, q).start()

    def to_x(t, dx):
        return remote(a.at[t, j], a.at[t, j], x_send.at[dx - 1, t], x_recv.at[dx - 1, t], x_peer(dx))

    def to_mate(t):
        return remote(a.at[t, j], a.at[t, j], c_send.at[t], c_recv.at[t], mate)

    def forward(t, dx):
        col = x_col(chips - dx)
        return remote(a.at[t, col], a.at[t, col], f_send.at[dx - 1, t], f_recv.at[dx - 1, t], mate)

    def arrived(slot, sem):
        pltpu.make_async_copy(slot, slot, sem).wait()

    def spread(t):
        arrived(a.at[t, j], s1_recv.at[t])
        for dx in range(1, chips):
            to_x(t, dx).start()
        to_mate(t).start()

    def relay(t):
        for dx in range(1, chips):
            arrived(a.at[t, x_col(chips - dx)], x_recv.at[dx - 1, t])
            forward(t, dx).start()

    def complete(t):
        arrived(a.at[t, x * CORES + 1 - core], c_recv.at[t])
        for dx in range(1, chips):
            col = lax.rem(x + chips - dx, chips) * CORES + 1 - core
            arrived(a.at[t, col], f_recv.at[dx - 1, t])

    def half(h):
        if aligned:
            return w[:, pl.ds(pl.multiple_of(h * nh, 128), nh)]
        return w[h]

    def y_copy(t, q):
        return remote(out_y.at[t, q], in_y.at[t, q], y_send.at[t, q], y_recv.at[t, q], across)

    def down(t, q):
        return remote(own.at[t, q], chain.at[t, q], z_send.at[t, q], z_recv.at[t, q], below)

    def up(t, q):
        return remote(own.at[t, q], chain.at[t + 1, q], z_send.at[t, q], z_recv.at[t + 1, q], above)

    def place(s):
        pair, q = s // (2 * cols), s % (2 * cols) // 2
        return jnp.where(s % 2 == 0, pair, rows - 1 - pair), q

    def multiply(s):
        t, q = place(s)
        block = a[t, q]
        out_y[t, q] = jnp.dot(block, half(1 - d), preferred_element_type=jnp.float32)
        own[t, q] = jnp.dot(block, half(d), preferred_element_type=jnp.float32)
        y_copy(t, q).start()

    def finish(s):
        t, q = place(s)
        arrived(in_y.at[t, q], y_recv.at[t, q])
        own[t, q] += in_y[t, q]

        @pl.when(jnp.logical_and(t <= r, r < rows - 1))
        def _():
            arrived(chain.at[t, q], z_recv.at[t, q])
            own[t, q] += chain[t, q]

        @pl.when(jnp.logical_and(t >= r, r > 0))
        def _():
            arrived(chain.at[t + 1, q], z_recv.at[t + 1, q])
            own[t, q] += chain[t + 1, q]

        pl.when(t < r)(lambda: down(t, q).start())
        pl.when(t > r)(lambda: up(t, q).start())

        @pl.when(t == r)
        def _():
            o_ref[pl.ds(pl.multiple_of(q * tq, tq), tq), :] = own[t, q].astype(o_ref.dtype)

    spread(0)
    spread(rows - 1)
    relay(0)
    relay(rows - 1)
    w_copy.wait()

    def step(s, carry):
        pair, at = s // (2 * cols), s % (2 * cols)

        @pl.when(at == 0)
        def _():
            complete(pair)
            complete(rows - 1 - pair)

        @pl.when(s < steps)
        def _():
            multiply(s)

        more = pair + 1 < rows // 2

        @pl.when(jnp.logical_and(more, at == 1))
        def _():
            spread(pair + 1)
            spread(rows - 2 - pair)

        @pl.when(jnp.logical_and(more, at == 4))
        def _():
            relay(pair + 1)
            relay(rows - 2 - pair)

        @pl.when(s >= LAG)
        def _():
            finish(s - LAG)

        return carry

    lax.fori_loop(0, steps, step, 0)

    def last(s, carry):
        finish(s)
        return carry

    lax.fori_loop(steps - LAG, steps, last, 0)

    for i in range(share):
        for q in range(cols):
            pl.when(jnp.logical_not(is_me(i, q)))(lambda i=i, q=q: first(i, q).wait_send())

    def drain(t, carry):
        for dx in range(1, chips):
            to_x(t, dx).wait_send()
            forward(t, dx).wait_send()
        to_mate(t).wait_send()
        for q in range(cols):
            y_copy(t, q).wait_send()
            pl.when(t != r)(lambda q=q: down(t, q).wait_send())
        return carry

    lax.fori_loop(0, rows, drain, 0)


def project(rows, cols, heads, w_out):
    tokens = heads.shape[0]
    kb, n = w_out.shape
    nh, tq = n // 2, tokens // cols
    chips = cols // CORES
    aligned = nh % 128 == 0
    w_shape = (kb, n)
    if not aligned:
        w_out = jnp.stack([w_out[:, :nh], w_out[:, nh:]])
        w_shape = (2, kb, nh)
    dma = pltpu.SemaphoreType.DMA
    f32 = jnp.float32
    return pl.pallas_call(
        functools.partial(kernel, rows, cols, aligned),
        out_shape=jax.ShapeDtypeStruct((tokens, nh), jnp.bfloat16),
        in_specs=[pl.BlockSpec(memory_space=pltpu.HBM)] * 2,
        out_specs=pl.BlockSpec(memory_space=pltpu.VMEM),
        scratch_shapes=[
            pltpu.VMEM(w_shape, jnp.bfloat16),
            pltpu.VMEM((rows, cols, tq, kb), jnp.bfloat16),
            pltpu.VMEM((rows, cols, tq, nh), f32),
            pltpu.VMEM((rows, cols, tq, nh), f32),
            pltpu.VMEM((rows, cols, tq, nh), f32),
            pltpu.VMEM((rows + 1, cols, tq, nh), f32),
            dma,
            dma((rows // cols, cols)), dma((rows,)),
            dma((chips - 1, rows)), dma((chips - 1, rows)),
            dma((rows,)), dma((rows,)),
            dma((chips - 1, rows)), dma((chips - 1, rows)),
            dma((rows, cols)), dma((rows, cols)),
            dma((rows, cols)), dma((rows + 1, cols)),
        ],
        compiler_params=pltpu.CompilerParams(
            collective_id=0, has_side_effects=True, vmem_limit_bytes=VMEM_BYTES
        ),
    )(heads, w_out)


def solution(mesh):
    rows, cols = mesh.shape["row"], mesh.shape["col"]

    def per_device(heads, w_out):
        tokens, n = heads.shape[0], w_out.shape[1]
        lanes = -(-n // 256) * 128
        slots = 17 * rows * tokens * lanes
        calls = 1
        while slots // calls > VMEM_BYTES // 2:
            calls *= 2
        size = tokens // calls
        parts = [
            project(rows, cols, heads[c * size:(c + 1) * size], w_out)
            for c in range(calls)
        ]
        return parts[0] if calls == 1 else jnp.concatenate(parts, axis=0)

    return jax.shard_map(
        per_device,
        mesh=mesh,
        in_specs=(P("row", ("depth", "col")), P(("depth", "row"), "col")),
        out_specs=P("row", ("col", "depth")),
        check_vma=False,
    )
```

```python
import functools

import jax
import jax.numpy as jnp
from jax import lax
from jax.experimental import pallas as pl
from jax.experimental.pallas import tpu as pltpu
from jax.sharding import PartitionSpec as P

MESH = pl.DeviceIdType.MESH
CORES = 2
LAG = 2
VMEM_BYTES = 66_000_000


def finishing(rows, r):
    downward = [(2 * t + rows - 1 - r, t) for t in range(r)]
    upward = [(2 * (rows - 1 - t) + r, t) for t in range(r + 1, rows)]
    return [t for _, t in sorted(downward + upward)] + [r]


def kernel(rows, cols, aligned, a_ref, w_ref, o_ref, w, a, own, out_y, in_y, chain,
           w_sem, s1_send, s1_recv, x_send, x_recv, c_send, c_recv, f_send, f_recv,
           y_send, y_recv, z_send, z_recv):
    r, j, d = lax.axis_index("row"), lax.axis_index("col"), lax.axis_index("depth")
    chips = cols // CORES
    x, core = j // CORES, j % CORES
    share = rows // cols
    tq, kb = a.shape[2], a.shape[3]
    nh = own.shape[3]
    steps = rows * cols
    mate = {"row": r, "col": x * CORES + 1 - core, "depth": d}
    across = {"row": r, "col": j, "depth": 1 - d}
    below = {"row": lax.rem(r + rows - 1, rows), "col": j, "depth": d}
    above = {"row": lax.rem(r + 1, rows), "col": j, "depth": d}
    source_col = r // share

    def x_col(dx):
        return lax.rem(x + dx, chips) * CORES + core

    def x_peer(dx):
        return {"row": r, "col": x_col(dx), "depth": d}

    w_copy = pltpu.make_async_copy(w_ref, w, w_sem)
    w_copy.start()

    barrier = pltpu.get_barrier_semaphore()

    def greet(device):
        pl.semaphore_signal(barrier, inc=1, device_id=device, device_id_type=MESH)

    for t in range(rows):
        pl.when(jnp.logical_or(r != t, source_col != j))(
            lambda t=t: greet({"row": t, "col": source_col, "depth": d})
        )
    for dx in range(1, chips):
        greet(x_peer(dx))
    greet(mate)
    greet(across)
    pl.when(r > 0)(lambda: greet(below))
    pl.when(r < rows - 1)(lambda: greet(above))
    pl.semaphore_wait(
        barrier,
        share * cols + chips
        + jnp.where(source_col != j, 1, 0)
        + jnp.where(r > 0, 1, 0)
        + jnp.where(r < rows - 1, 1, 0),
    )

    def remote(src, dst, send, recv, device):
        return pltpu.make_async_remote_copy(
            src_ref=src, dst_ref=dst, send_sem=send, recv_sem=recv,
            device_id=device, device_id_type=MESH,
        )

    def first(i, q):
        target = {"row": j * share + i, "col": q, "depth": d}
        source = a_ref.at[pl.ds(q * tq, tq), pl.ds(i * kb, kb)]
        return remote(source, a.at[r, q], s1_send.at[i, q], s1_recv.at[r], target)

    def is_me(i, q):
        return jnp.logical_and(r == j * share + i, j == q)

    for i in range(share):
        for q in range(cols):
            @pl.when(is_me(i, q))
            def _():
                pltpu.make_async_copy(
                    a_ref.at[pl.ds(q * tq, tq), pl.ds(i * kb, kb)],
                    a.at[r, q], s1_recv.at[r],
                ).start()

            @pl.when(jnp.logical_not(is_me(i, q)))
            def _():
                first(i, q).start()

    def to_x(t, dx):
        return remote(a.at[t, j], a.at[t, j], x_send.at[dx - 1, t], x_recv.at[dx - 1, t], x_peer(dx))

    def to_mate(t):
        return remote(a.at[t, j], a.at[t, j], c_send.at[t], c_recv.at[t], mate)

    def forward(t, dx):
        col = x_col(chips - dx)
        return remote(a.at[t, col], a.at[t, col], f_send.at[dx - 1, t], f_recv.at[dx - 1, t], mate)

    def arrived(slot, sem):
        pltpu.make_async_copy(slot, slot, sem).wait()

    def spread(t):
        arrived(a.at[t, j], s1_recv.at[t])
        for dx in range(1, chips):
            to_x(t, dx).start()
        to_mate(t).start()

    def relay(t):
        for dx in range(1, chips):
            arrived(a.at[t, x_col(chips - dx)], x_recv.at[dx - 1, t])
            forward(t, dx).start()

    def half(h):
        if aligned:
            return w[:, pl.ds(pl.multiple_of(h * nh, 128), nh)]
        return w[h]

    def y_copy(t, q):
        return remote(out_y.at[t, q], in_y.at[t, q], y_send.at[t, q], y_recv.at[t, q], across)

    def down(t, q):
        return remote(own.at[t, q], chain.at[t, q], z_send.at[t, q], z_recv.at[t, q], below)

    def up(t, q):
        return remote(own.at[t, q], chain.at[t + 1, q], z_send.at[t, q], z_recv.at[t + 1, q], above)

    order = []
    for p in range(rows):
        block = jnp.int32(0)
        for row in range(rows):
            block = jnp.where(r == row, finishing(rows, row)[p], block)
        order.append(block)

    def pick(p):
        block = order[0]
        for n in range(1, rows):
            block = jnp.where(p == n, order[n], block)
        return block

    def column(k):
        chip = lax.rem(x + chips - k // CORES, chips)
        return chip * CORES + jnp.where(k % CORES == 0, core, 1 - core)

    def multiply(t, q):
        block = a[t, q]
        out_y[t, q] = jnp.dot(block, half(1 - d), preferred_element_type=jnp.float32)
        own[t, q] = jnp.dot(block, half(d), preferred_element_type=jnp.float32)
        y_copy(t, q).start()

    def finish(s):
        t, q = pick(s // cols), column(s % cols)
        arrived(in_y.at[t, q], y_recv.at[t, q])
        own[t, q] += in_y[t, q]

        @pl.when(jnp.logical_and(t <= r, r < rows - 1))
        def _():
            arrived(chain.at[t, q], z_recv.at[t, q])
            own[t, q] += chain[t, q]

        @pl.when(jnp.logical_and(t >= r, r > 0))
        def _():
            arrived(chain.at[t + 1, q], z_recv.at[t + 1, q])
            own[t, q] += chain[t + 1, q]

        pl.when(t < r)(lambda: down(t, q).start())
        pl.when(t > r)(lambda: up(t, q).start())

        @pl.when(t == r)
        def _():
            o_ref[pl.ds(pl.multiple_of(q * tq, tq), tq), :] = own[t, q].astype(o_ref.dtype)

    spread(r)
    w_copy.wait()

    def step(s, carry):
        p, k = s // cols, s % cols
        t = pick(lax.rem(p + rows - 1, rows))

        @pl.when(k == 1)
        def _():
            arrived(a.at[t, column(1)], c_recv.at[t])

        pl.when(k == CORES)(lambda: relay(t))
        for dx in range(1, chips):
            @pl.when(k == CORES * dx + 1)
            def _():
                arrived(a.at[t, column(CORES * dx + 1)], f_recv.at[dx - 1, t])

        multiply(t, column(k))

        @pl.when(s == cols - 1)
        def _():
            for n in range(rows - 1):
                spread(order[n])

        pl.when(s >= cols + LAG)(lambda: finish(s - cols - LAG))
        return carry

    lax.fori_loop(0, steps, step, 0)

    def last(s, carry):
        finish(s)
        return carry

    lax.fori_loop(steps - cols - LAG, steps, last, 0)

    for i in range(share):
        for q in range(cols):
            pl.when(jnp.logical_not(is_me(i, q)))(lambda i=i, q=q: first(i, q).wait_send())

    def drain(t, carry):
        for dx in range(1, chips):
            to_x(t, dx).wait_send()
            forward(t, dx).wait_send()
        to_mate(t).wait_send()
        for q in range(cols):
            y_copy(t, q).wait_send()
            pl.when(t != r)(lambda q=q: down(t, q).wait_send())
        return carry

    lax.fori_loop(0, rows, drain, 0)


def project(rows, cols, heads, w_out):
    tokens = heads.shape[0]
    kb, n = w_out.shape
    nh, tq = n // 2, tokens // cols
    chips = cols // CORES
    aligned = nh % 128 == 0
    w_shape = (kb, n)
    if not aligned:
        w_out = jnp.stack([w_out[:, :nh], w_out[:, nh:]])
        w_shape = (2, kb, nh)
    dma = pltpu.SemaphoreType.DMA
    f32 = jnp.float32
    return pl.pallas_call(
        functools.partial(kernel, rows, cols, aligned),
        out_shape=jax.ShapeDtypeStruct((tokens, nh), jnp.bfloat16),
        in_specs=[pl.BlockSpec(memory_space=pltpu.HBM)] * 2,
        out_specs=pl.BlockSpec(memory_space=pltpu.VMEM),
        scratch_shapes=[
            pltpu.VMEM(w_shape, jnp.bfloat16),
            pltpu.VMEM((rows, cols, tq, kb), jnp.bfloat16),
            pltpu.VMEM((rows, cols, tq, nh), f32),
            pltpu.VMEM((rows, cols, tq, nh), f32),
            pltpu.VMEM((rows, cols, tq, nh), f32),
            pltpu.VMEM((rows + 1, cols, tq, nh), f32),
            dma,
            dma((rows // cols, cols)), dma((rows,)),
            dma((chips - 1, rows)), dma((chips - 1, rows)),
            dma((rows,)), dma((rows,)),
            dma((chips - 1, rows)), dma((chips - 1, rows)),
            dma((rows, cols)), dma((rows, cols)),
            dma((rows, cols)), dma((rows + 1, cols)),
        ],
        compiler_params=pltpu.CompilerParams(
            collective_id=0, has_side_effects=True, vmem_limit_bytes=VMEM_BYTES
        ),
    )(heads, w_out)


def solution(mesh):
    rows, cols = mesh.shape["row"], mesh.shape["col"]

    def per_device(heads, w_out):
        tokens, n = heads.shape[0], w_out.shape[1]
        lanes = -(-n // 256) * 128
        slots = 17 * rows * tokens * lanes
        calls = 1
        while slots // calls > VMEM_BYTES // 2:
            calls *= 2
        size = tokens // calls
        parts = [
            project(rows, cols, heads[c * size:(c + 1) * size], w_out)
            for c in range(calls)
        ]
        return parts[0] if calls == 1 else jnp.concatenate(parts, axis=0)

    return jax.shard_map(
        per_device,
        mesh=mesh,
        in_specs=(P("row", ("depth", "col")), P(("depth", "row"), "col")),
        out_specs=P("row", ("col", "depth")),
        check_vma=False,
    )
```

```python
import functools

import jax
import jax.numpy as jnp
from jax import lax
from jax.experimental import pallas as pl
from jax.experimental.pallas import tpu as pltpu
from jax.sharding import PartitionSpec as P

MESH = pl.DeviceIdType.MESH
CORES = 2
LAG = 2
VMEM_BYTES = 66_000_000


def finishing(rows, r):
    downward = [(2 * t + rows - 1 - r, t) for t in range(r)]
    upward = [(2 * (rows - 1 - t) + r, t) for t in range(r + 1, rows)]
    return [t for _, t in sorted(downward + upward)] + [r]


def kernel(rows, cols, aligned, a_ref, w_ref, o_ref, w, a, own, out_y, in_y, chain,
           w_sem, s1_send, s1_recv, x_send, x_recv, c_send, c_recv, f_send, f_recv,
           y_send, y_recv, z_send, z_recv):
    r, j, d = lax.axis_index("row"), lax.axis_index("col"), lax.axis_index("depth")
    chips = cols // CORES
    x, core = j // CORES, j % CORES
    share = rows // cols
    tq, kb = a.shape[2], a.shape[3]
    nh = own.shape[3]
    steps = rows * cols
    mate = {"row": r, "col": x * CORES + 1 - core, "depth": d}
    across = {"row": r, "col": j, "depth": 1 - d}
    below = {"row": lax.rem(r + rows - 1, rows), "col": j, "depth": d}
    above = {"row": lax.rem(r + 1, rows), "col": j, "depth": d}
    source_col = r // share

    def x_col(dx):
        return lax.rem(x + dx, chips) * CORES + core

    def x_peer(dx):
        return {"row": r, "col": x_col(dx), "depth": d}

    w_copy = pltpu.make_async_copy(w_ref, w, w_sem)
    w_copy.start()

    barrier = pltpu.get_barrier_semaphore()

    def greet(device):
        pl.semaphore_signal(barrier, inc=1, device_id=device, device_id_type=MESH)

    for t in range(rows):
        pl.when(jnp.logical_or(r != t, source_col != j))(
            lambda t=t: greet({"row": t, "col": source_col, "depth": d})
        )
    for dx in range(1, chips):
        greet(x_peer(dx))
    greet(mate)
    greet(across)
    pl.when(r > 0)(lambda: greet(below))
    pl.when(r < rows - 1)(lambda: greet(above))
    pl.semaphore_wait(
        barrier,
        share * cols + chips
        + jnp.where(source_col != j, 1, 0)
        + jnp.where(r > 0, 1, 0)
        + jnp.where(r < rows - 1, 1, 0),
    )

    def remote(src, dst, send, recv, device):
        return pltpu.make_async_remote_copy(
            src_ref=src, dst_ref=dst, send_sem=send, recv_sem=recv,
            device_id=device, device_id_type=MESH,
        )

    def first(i, q):
        target = {"row": j * share + i, "col": q, "depth": d}
        source = a_ref.at[pl.ds(q * tq, tq), pl.ds(i * kb, kb)]
        return remote(source, a.at[r, q], s1_send.at[i, q], s1_recv.at[r], target)

    def is_me(i, q):
        return jnp.logical_and(r == j * share + i, j == q)

    for i in range(share):
        for q in range(cols):
            @pl.when(is_me(i, q))
            def _():
                pltpu.make_async_copy(
                    a_ref.at[pl.ds(q * tq, tq), pl.ds(i * kb, kb)],
                    a.at[r, q], s1_recv.at[r],
                ).start()

            @pl.when(jnp.logical_not(is_me(i, q)))
            def _():
                first(i, q).start()

    def to_x(t, dx):
        return remote(a.at[t, j], a.at[t, j], x_send.at[dx - 1, t], x_recv.at[dx - 1, t], x_peer(dx))

    def to_mate(t):
        return remote(a.at[t, j], a.at[t, j], c_send.at[t], c_recv.at[t], mate)

    def forward(t, dx):
        col = x_col(chips - dx)
        return remote(a.at[t, col], a.at[t, col], f_send.at[dx - 1, t], f_recv.at[dx - 1, t], mate)

    def arrived(slot, sem):
        pltpu.make_async_copy(slot, slot, sem).wait()

    def spread(t):
        arrived(a.at[t, j], s1_recv.at[t])
        for dx in range(1, chips):
            to_x(t, dx).start()
        to_mate(t).start()

    def relay(t):
        for dx in range(1, chips):
            arrived(a.at[t, x_col(chips - dx)], x_recv.at[dx - 1, t])
            forward(t, dx).start()

    def half(h):
        if aligned:
            return w[:, pl.ds(pl.multiple_of(h * nh, 128), nh)]
        return w[h]

    def y_copy(t, q):
        return remote(out_y.at[t, q], in_y.at[t, q], y_send.at[t, q], y_recv.at[t, q], across)

    def down(t, q):
        return remote(own.at[t, q], chain.at[t, q], z_send.at[t, q], z_recv.at[t, q], below)

    def up(t, q):
        return remote(own.at[t, q], chain.at[t + 1, q], z_send.at[t, q], z_recv.at[t + 1, q], above)

    order = []
    for p in range(rows):
        block = jnp.int32(0)
        for row in range(rows):
            block = jnp.where(r == row, finishing(rows, row)[p], block)
        order.append(block)

    def pick(p):
        block = order[0]
        for n in range(1, rows):
            block = jnp.where(p == n, order[n], block)
        return block

    def place(n):
        k = n // (CORES * (rows - 1)) * CORES + n % CORES
        return n // CORES % (rows - 1), k

    def column(k):
        chip = lax.rem(x + chips - k // CORES, chips)
        return chip * CORES + jnp.where(k % CORES == 0, core, 1 - core)

    def multiply(t, q):
        block = a[t, q]
        out_y[t, q] = jnp.dot(block, half(1 - d), preferred_element_type=jnp.float32)
        own[t, q] = jnp.dot(block, half(d), preferred_element_type=jnp.float32)
        y_copy(t, q).start()

    def finish(s):
        p, k = place(s)
        mine = s >= steps - cols
        t = jnp.where(mine, r, pick(p))
        q = column(jnp.where(mine, s - (steps - cols), k))
        arrived(in_y.at[t, q], y_recv.at[t, q])
        own[t, q] += in_y[t, q]

        @pl.when(jnp.logical_and(t <= r, r < rows - 1))
        def _():
            arrived(chain.at[t, q], z_recv.at[t, q])
            own[t, q] += chain[t, q]

        @pl.when(jnp.logical_and(t >= r, r > 0))
        def _():
            arrived(chain.at[t + 1, q], z_recv.at[t + 1, q])
            own[t, q] += chain[t + 1, q]

        pl.when(t < r)(lambda: down(t, q).start())
        pl.when(t > r)(lambda: up(t, q).start())

        @pl.when(t == r)
        def _():
            o_ref[pl.ds(pl.multiple_of(q * tq, tq), tq), :] = own[t, q].astype(o_ref.dtype)

    w_copy.wait()

    def step(s, carry):
        p, k = place(s - cols)
        mine = s < cols
        t = jnp.where(mine, r, pick(p))
        k = jnp.where(mine, s, k)

        pl.when(k == 0)(lambda: spread(t))

        @pl.when(k == 1)
        def _():
            arrived(a.at[t, column(1)], c_recv.at[t])

        pl.when(k == CORES)(lambda: relay(t))
        for dx in range(1, chips):
            @pl.when(k == CORES * dx + 1)
            def _():
                arrived(a.at[t, column(CORES * dx + 1)], f_recv.at[dx - 1, t])

        multiply(t, column(k))

        pl.when(s >= cols + LAG)(lambda: finish(s - cols - LAG))
        return carry

    lax.fori_loop(0, steps, step, 0)

    def last(s, carry):
        finish(s)
        return carry

    lax.fori_loop(steps - cols - LAG, steps, last, 0)

    for i in range(share):
        for q in range(cols):
            pl.when(jnp.logical_not(is_me(i, q)))(lambda i=i, q=q: first(i, q).wait_send())

    def drain(t, carry):
        for dx in range(1, chips):
            to_x(t, dx).wait_send()
            forward(t, dx).wait_send()
        to_mate(t).wait_send()
        for q in range(cols):
            y_copy(t, q).wait_send()
            pl.when(t != r)(lambda q=q: down(t, q).wait_send())
        return carry

    lax.fori_loop(0, rows, drain, 0)


def project(rows, cols, heads, w_out):
    tokens = heads.shape[0]
    kb, n = w_out.shape
    nh, tq = n // 2, tokens // cols
    chips = cols // CORES
    aligned = nh % 128 == 0
    w_shape = (kb, n)
    if not aligned:
        w_out = jnp.stack([w_out[:, :nh], w_out[:, nh:]])
        w_shape = (2, kb, nh)
    dma = pltpu.SemaphoreType.DMA
    f32 = jnp.float32
    return pl.pallas_call(
        functools.partial(kernel, rows, cols, aligned),
        out_shape=jax.ShapeDtypeStruct((tokens, nh), jnp.bfloat16),
        in_specs=[pl.BlockSpec(memory_space=pltpu.HBM)] * 2,
        out_specs=pl.BlockSpec(memory_space=pltpu.VMEM),
        scratch_shapes=[
            pltpu.VMEM(w_shape, jnp.bfloat16),
            pltpu.VMEM((rows, cols, tq, kb), jnp.bfloat16),
            pltpu.VMEM((rows, cols, tq, nh), f32),
            pltpu.VMEM((rows, cols, tq, nh), f32),
            pltpu.VMEM((rows, cols, tq, nh), f32),
            pltpu.VMEM((rows + 1, cols, tq, nh), f32),
            dma,
            dma((rows // cols, cols)), dma((rows,)),
            dma((chips - 1, rows)), dma((chips - 1, rows)),
            dma((rows,)), dma((rows,)),
            dma((chips - 1, rows)), dma((chips - 1, rows)),
            dma((rows, cols)), dma((rows, cols)),
            dma((rows, cols)), dma((rows + 1, cols)),
        ],
        compiler_params=pltpu.CompilerParams(
            collective_id=0, has_side_effects=True, vmem_limit_bytes=VMEM_BYTES
        ),
    )(heads, w_out)


def solution(mesh):
    rows, cols = mesh.shape["row"], mesh.shape["col"]

    def per_device(heads, w_out):
        tokens, n = heads.shape[0], w_out.shape[1]
        lanes = -(-n // 256) * 128
        slots = 17 * rows * tokens * lanes
        calls = 1
        while slots // calls > VMEM_BYTES // 2:
            calls *= 2
        size = tokens // calls
        parts = [
            project(rows, cols, heads[c * size:(c + 1) * size], w_out)
            for c in range(calls)
        ]
        return parts[0] if calls == 1 else jnp.concatenate(parts, axis=0)

    return jax.shard_map(
        per_device,
        mesh=mesh,
        in_specs=(P("row", ("depth", "col")), P(("depth", "row"), "col")),
        out_specs=P("row", ("col", "depth")),
        check_vma=False,
    )
```
